128 devices in a mesh: py: 16 (over x, y_hi, core), pz: 8 (over z, y_lo).
Axes of the slice: x: 4, y: 4 (y_hi: 2, y_lo: 2; y = y_hi * 2 + y_lo), z: 4, core: 2. Of those that a mesh axis runs over, the one named last changes fastest.
Arguments:
- velocity: float32 [3, 128, 128, 2048], P(None, ('py', 'pz')), may hold values from -6 to 6
- fluid: float32 [128, 128, 2048], P(('py', 'pz')), may hold values from 0.1 to 1
- pressure: float32 [128, 128, 2048], P(None, 'pz', 'py'), may hold values from -4 to 4
Outputs:
- projected: float32 [3, 128, 128, 2048], P(None, ('py', 'pz'))
- divergence: float32 [128, 128, 2048], P(None, 'pz', 'py')
The draws below stay inside these ranges and needn't reach their ends.
All inputs are finite; a program needn't handle non-finite values.
Results may differ from the reference program's by a relative error of at most 0.00002.
Values sent between devices are 32-bit elements; how exact they have to be, the bound alone decides.
No kernel may reach another device: no remote copies, remote signals or barrier semaphores. Data moves between devices by JAX's collectives and lax.ppermute only.
A program may use at most 64 MiB of HBM per device.

```python
import jax
import jax.numpy as jnp
from jax import lax

NY = 2048
NZ = 128
NX = 128


def shard_levels(rng, shape, shards, low, high):
    loudness, own = 1.0, jax.random.fold_in(rng, 6)
    for dim, shards_of in shards:
        draws = jnp.exp(jax.random.uniform(jax.random.fold_in(own, dim), (shards_of,), jnp.float32, low / len(shards), high / len(shards)))
        loudness = loudness * jnp.repeat(draws, shape[dim] // shards_of).reshape([-1 if axis == dim else 1 for axis in range(len(shape))])
    return loudness


def bell_draw(key, shape, deviation, limit, cuts=(), held_as=jnp.bfloat16):
    array = jax.random.normal(key, shape, jnp.float32) * deviation
    if len(cuts) > 0:
        array = shard_levels(key, shape, cuts, -0.22, 0.18) * array
    return jnp.clip(array, min=-limit, max=limit).astype(held_as)


def setup_inputs(seed: int = 0) -> dict:
    splits = jax.random.split(jax.random.key(seed), 4)
    velocity = bell_draw(splits[0], (3, NX, NZ, NY), 1.0, 6.0, ((1, 128),), jnp.float32)
    fluid = jnp.clip(0.1 + 0.9 * jax.random.uniform(splits[1], (NX, NZ, NY), jnp.float32) ** shard_levels(splits[1], (NX, NZ, NY), ((0, 128),), -0.2, 0.2), 0.1, 1.0)
    pressure = bell_draw(splits[2], (NX, NZ, NY), 0.5, 4.0, ((1, 8), (2, 16)), jnp.float32)
    return {"velocity": velocity, "fluid": fluid, "pressure": pressure}


def face_update(component, fluid, pressure, axis):
    index = lax.broadcasted_iota(jnp.int32, fluid.shape, axis)
    fluid_prev = jnp.roll(fluid, 1, axis)
    pressure_prev = jnp.roll(pressure, 1, axis)
    weight = jnp.where(index == 0, jnp.float32(0.0), 0.5 * (fluid + fluid_prev))
    return weight * (component - (pressure - pressure_prev))


def forward_difference(updated, axis):
    index = lax.broadcasted_iota(jnp.int32, updated.shape, axis)
    following = jnp.where(index == updated.shape[axis] - 1, jnp.float32(0.0), jnp.roll(updated, -1, axis))
    return following - updated


def reference(velocity, fluid, pressure):
    parts = []
    divergence = jnp.zeros(fluid.shape, jnp.float32)
    for axis in range(3):
        updated = face_update(velocity[axis], fluid, pressure, axis)
        divergence = divergence + forward_difference(updated, axis)
        parts.append(updated)
    return jnp.stack(parts, 0), divergence
```

```python
import jax
import jax.numpy as jnp
from jax import lax
from jax.experimental import pallas as pl
from jax.experimental.pallas import tpu as pltpu
from jax.sharding import PartitionSpec as P

BOTH = ("py", "pz")
F32 = jnp.float32
HBM = pl.BlockSpec(memory_space=pltpu.HBM)
VMEM = pltpu.VMEM
DMA = pltpu.SemaphoreType.DMA


def call(kernel, outs, ins, scratch, mib, moved, **more):
    spec = {pltpu.HBM: HBM, VMEM: pl.BlockSpec(memory_space=VMEM)}
    return pl.pallas_call(
        kernel,
        out_shape=tuple(space(shape, F32) for shape, space in outs),
        in_specs=[spec[space] for _, space in ins],
        out_specs=tuple(spec[space] for _, space in outs),
        scratch_shapes=scratch,
        compiler_params=pltpu.CompilerParams(vmem_limit_bytes=mib * 1024 * 1024),
        cost_estimate=pl.CostEstimate(flops=moved, bytes_accessed=moved, transcendentals=0),
        **more,
    )(*(pltpu.with_memory_space_constraint(x, space) for x, space in ins))


def start(copies):
    for c in copies:
        c.start()


def wait(copies):
    for c in copies:
        c.wait()


def pack_kernel(f, v, p, out, sem_f, sem_v, sem_p):
    ny, ty = out.shape[0], out.shape[-1]
    copy = pltpu.make_async_copy
    loads = [copy(p, out.at[:, :, 2], sem_p)]
    for i in range(ny):
        cols = pl.ds(i * ty, ty)
        loads.append(copy(f.at[:, :, cols], out.at[i, :, 0], sem_f.at[i]))
        loads.append(copy(v.at[0, :, :, cols], out.at[i, :, 1], sem_v.at[i]))
    start(loads)
    wait(loads)


def middle_kernel(r, p_h, f_h, v_h, op, proj_h, px_h, p, f, v, zy, px, sem_p, sem_f, sem_v, sem_x, sem_zy):
    ny, nz, _, tz, ty = r.shape
    depth = nz * tz
    copy = pltpu.make_async_copy
    loads = []
    for i in range(ny):
        cols = pl.ds(i * ty, ty)
        loads.append((
            copy(p_h.at[i], p.at[i], sem_p.at[i]),
            copy(f_h.at[:, cols], f.at[i], sem_f.at[i]),
            copy(v_h.at[pl.ds(1, 2), :, cols], v.at[i], sem_v.at[i]),
        ))
        start(loads[-1])
    row = lax.broadcasted_iota(jnp.int32, (depth, ty), 0)
    lane = lax.broadcasted_iota(jnp.int32, (depth, ty), 1)
    stores = []
    before = None
    for i in range(ny):
        wait(loads[i])
        for j in range(nz):
            if i == 0 and j == 0:
                op[0, 0, 0] = px[0, 0] = jnp.zeros((tz, ty), F32)
                continue
            a, b = (i, j - 1) if j else (i - 1, nz - 1)
            weight = 0.5 * (r[i, j, 0] + r[a, b, 0])
            op[i, j, 0] = px[i, j] = weight * (r[i, j, 1] - (p[i, j] - p[a, b]))
        stores.append(copy(px.at[i], px_h.at[i], sem_x.at[i]))
        stores[-1].start()
        pres = r[i, :, 2].reshape(depth, ty)
        fluid = f[i]
        weight = jnp.where(row == 0, 0.0, 0.5 * (fluid + pltpu.roll(fluid, 1, 0)))
        pz = weight * (v[i, 0] - (pres - pltpu.roll(pres, 1, 0)))
        zy[i, 0] = pz
        dz = jnp.where(row == depth - 1, 0.0, pltpu.roll(pz, depth - 1, 0)) - pz
        rp, rf = pltpu.roll(pres, 1, 1), pltpu.roll(fluid, 1, 1)
        if i == 0:
            weight = jnp.where(lane == 0, 0.0, 0.5 * (fluid + rf))
            left = rp
        else:
            weight = 0.5 * (fluid + jnp.where(lane == 0, before[1], rf))
            left = jnp.where(lane == 0, before[0], rp)
        py = weight * (v[i, 1] - (pres - left))
        zy[i, 1] = py
        stores.append(copy(zy.at[i], proj_h.at[pl.ds(1, 2), :, pl.ds(i * ty, ty)], sem_zy.at[i]))
        stores[-1].start()
        op[i, :, 1] = (dz - py).reshape(nz, tz, ty)
        ry = pltpu.roll(py, ty - 1, 1)
        if i:
            op[i - 1, :, 1] += jnp.where(lane == ty - 1, ry, before[2]).reshape(nz, tz, ty)
        before = rp, rf, ry
    op[ny - 1, :, 1] += jnp.where(lane == ty - 1, 0.0, before[2]).reshape(nz, tz, ty)
    wait(stores)


def final_kernel(r, px_h, proj_in, proj_h, div_h, px, div, sem_x, sem_p, sem_d):
    del proj_in
    ny, nz, _, tz, ty = r.shape
    copy = pltpu.make_async_copy
    loads = [copy(px_h.at[i], px.at[i], sem_x.at[i]) for i in range(ny)]
    start(loads)
    stores = [copy(r.at[i, :, 0], proj_h.at[0, :, :, pl.ds(i * ty, ty)], sem_p.at[i]) for i in range(ny)]
    start(stores)
    loads[0].wait()
    for i in range(ny):
        if i + 1 < ny:
            loads[i + 1].wait()
        for j in range(nz):
            if j < nz - 1:
                after = px[i, j + 1]
            else:
                after = px[i + 1, 0] if i < ny - 1 else 0.0
            div[i, j] = r[i, j, 1] + (after - px[i, j])
        stores.append(copy(div.at[i], div_h.at[i], sem_d.at[i]))
        stores[-1].start()
    wait(stores)


def exchange(blocks):
    ny, nz = blocks.shape[:2]
    flat = blocks.reshape(ny * nz, *blocks.shape[2:])
    return lax.all_to_all(flat, BOTH, split_axis=0, concat_axis=0, tiled=True).reshape(blocks.shape)


def on_device(velocity, fluid, pressure):
    ny = lax.axis_size("py")
    nz = lax.axis_size("pz")
    _, depth, across = fluid.shape
    tz, ty = pressure.shape[1:]
    plane = depth * across * 4
    p4 = pressure.reshape(ny, nz, tz, ty)
    tiles = (ny, nz, tz, ty)
    sems = DMA((ny,))
    far = pltpu.HBM

    (packed,) = call(
        pack_kernel, [((ny, nz, 3, tz, ty), VMEM)],
        [(fluid.reshape(nz, tz, across), far), (velocity.reshape(3, nz, tz, across), far), (p4, far)],
        [sems, sems, DMA], 8, 3 * plane,
    )
    first = exchange(packed)
    op, partial, px = call(
        middle_kernel, [((ny, nz, 2, tz, ty), VMEM), ((3, depth, across), far), (tiles, far)],
        [(first, VMEM), (p4, far), (fluid.reshape(depth, across), far), (velocity.reshape(3, depth, across), far)],
        [VMEM(tiles, F32), VMEM((ny, depth, ty), F32), VMEM((ny, 2, depth, ty), F32), VMEM((ny, 2, depth, ty), F32),
         VMEM(tiles, F32)] + [sems] * 5, 32, 7 * plane,
    )
    second = exchange(op)
    projected, divergence = call(
        final_kernel, [((3, nz, tz, across), far), (tiles, far)],
        [(second, VMEM), (px, far), (partial.reshape(3, nz, tz, across), far)],
        [VMEM(tiles, F32)] * 2 + [sems] * 3, 16, 3 * plane,
        input_output_aliases={2: 0},
    )
    return projected.reshape(velocity.shape), divergence.reshape(pressure.shape)


def solution(mesh):
    placed = (P(None, BOTH, None, None), P(BOTH, None, None), P(None, "pz", "py"))
    return jax.shard_map(
        on_device,
        mesh=mesh,
        in_specs=placed,
        out_specs=(P(None, BOTH, None, None), P(None, "pz", "py")),
        check_vma=False,
    )
```

```python
import jax
import jax.numpy as jnp
from jax import lax
from jax.experimental import pallas as pl
from jax.experimental.pallas import tpu as pltpu
from jax.sharding import PartitionSpec as P

ANY = pl.ANY
BOTH = ("py", "pz")
F32 = jnp.float32
HBM = pl.BlockSpec(memory_space=pltpu.HBM)
VMEM = pltpu.VMEM
DMA = pltpu.SemaphoreType.DMA


def call(kernel, outs, ins, scratch, mib, moved, **more):
    spec = {ANY: HBM, pltpu.HBM: HBM, None: pl.BlockSpec(memory_space=VMEM), VMEM: pl.BlockSpec(memory_space=VMEM)}
    return pl.pallas_call(
        kernel,
        out_shape=tuple((space or jax.ShapeDtypeStruct)(shape, F32) for shape, space in outs),
        in_specs=[spec[space] for _, space in ins],
        out_specs=tuple(spec[space] for _, space in outs),
        scratch_shapes=scratch,
        compiler_params=pltpu.CompilerParams(vmem_limit_bytes=mib * 1024 * 1024),
        cost_estimate=pl.CostEstimate(flops=moved, bytes_accessed=moved, transcendentals=0),
        **more,
    )(*(x if space in (None, ANY) else pltpu.with_memory_space_constraint(x, space) for x, space in ins))


def start(copies):
    for c in copies:
        c.start()


def wait(copies):
    for c in copies:
        c.wait()


def pack_kernel(f_h, v_h, p_h, out, p, wz, wy, f, v, sem_f, sem_v, sem_p):
    ny, nz, _, tz, ty = out.shape
    depth = nz * tz
    copy = pltpu.make_async_copy
    part = nz // 4
    rows = [pl.ds(k * part * tz, part * tz) for k in range(4)]
    loads_f = [copy(f_h.at[k], f.at[k], sem_f.at[i]) for i, k in enumerate(rows)]
    loads_v = [copy(v_h.at[0, k], v.at[k], sem_v.at[i]) for i, k in enumerate(rows)]
    load_p = copy(p_h, p, sem_p)
    start(loads_f)
    load_p.start()
    start(loads_v)
    row = lax.broadcasted_iota(jnp.int32, (depth, ty), 0)
    lane = lax.broadcasted_iota(jnp.int32, (depth, ty), 1)
    before = None
    wait(loads_f)
    for i in range(ny):
        fluid = f[:, pl.ds(i * ty, ty)]
        out[i, :, 0] = fluid.reshape(nz, tz, ty)
        wz[i] = jnp.where(row == 0, 0.0, 0.5 * (fluid + pltpu.roll(fluid, 1, 0)))
        turned = pltpu.roll(fluid, 1, 1)
        if i:
            wy[i] = 0.5 * (fluid + jnp.where(lane == 0, before, turned))
        else:
            wy[i] = jnp.where(lane == 0, 0.0, 0.5 * (fluid + turned))
        before = turned
    load_p.wait()
    for i in range(ny):
        out[i, :, 2] = p[i]
    for k in range(4):
        loads_v[k].wait()
        for i in range(ny):
            out[i, k * part : (k + 1) * part, 1] = v[rows[k], pl.ds(i * ty, ty)].reshape(part, tz, ty)


def middle_kernel(r, p, wz, wy, v, op, proj_h, px, faces, sems):
    ny, nz, _, tz, ty = r.shape
    depth = nz * tz
    row = lax.broadcasted_iota(jnp.int32, (depth, ty), 0)
    lane = lax.broadcasted_iota(jnp.int32, (depth, ty), 1)
    before = None
    stores = []
    for i in range(ny):
        for j in range(nz):
            if i == 0 and j == 0:
                op[0, 0, 0] = px[0, 0] = jnp.zeros((tz, ty), F32)
                continue
            a, b = (i, j - 1) if j else (i - 1, nz - 1)
            weight = 0.5 * (r[i, j, 0] + r[a, b, 0])
            op[i, j, 0] = px[i, j] = weight * (r[i, j, 1] - (p[i, j] - p[a, b]))
        cols = pl.ds(i * ty, ty)
        pres = r[i, :, 2].reshape(depth, ty)
        pz = wz[i] * (v[1, :, cols] - (pres - pltpu.roll(pres, 1, 0)))
        faces[0, :, cols] = pz
        dz = jnp.where(row == depth - 1, 0.0, pltpu.roll(pz, depth - 1, 0)) - pz
        rp = pltpu.roll(pres, 1, 1)
        left = jnp.where(lane == 0, before[0], rp) if i else rp
        py = wy[i] * (v[2, :, cols] - (pres - left))
        faces[1, :, cols] = py
        op[i, :, 1] = (dz - py).reshape(nz, tz, ty)
        if i % 4 == 3:
            done = pl.ds((i - 3) * ty, 4 * ty)
            stores.append(pltpu.make_async_copy(faces.at[:, :, done], proj_h.at[pl.ds(1, 2), :, done], sems.at[i // 4]))
            stores[-1].start()
        ry = pltpu.roll(py, ty - 1, 1)
        if i:
            op[i - 1, :, 1] += jnp.where(lane == ty - 1, ry, before[1]).reshape(nz, tz, ty)
        before = rp, ry
    op[ny - 1, :, 1] += jnp.where(lane == ty - 1, 0.0, before[1]).reshape(nz, tz, ty)
    wait(stores)


def final_kernel(r, px, faces, proj_h, div_h, first, div, sem_p, sem_d):
    del faces
    ny, nz, _, tz, ty = r.shape
    copy = pltpu.make_async_copy
    part = nz // 4
    stores = []
    for k in range(4):
        for j in range(k * part, (k + 1) * part):
            for i in range(ny):
                first[j, :, i * ty : (i + 1) * ty] = r[i, j, 0]
        rows = pl.ds(k * part, part)
        stores.append(copy(first.at[rows], proj_h.at[0, rows], sem_p.at[k]))
        stores[-1].start()
    quarter = ny // 4
    for k in range(4):
        for i in range(k * quarter, (k + 1) * quarter):
            for j in range(nz):
                if j < nz - 1:
                    after = px[i, j + 1]
                else:
                    after = px[i + 1, 0] if i < ny - 1 else 0.0
                div[i, j] = r[i, j, 1] + (after - px[i, j])
        rows = pl.ds(k * quarter, quarter)
        stores.append(copy(div.at[rows], div_h.at[rows], sem_d.at[k]))
        stores[-1].start()
    wait(stores)


def exchange(blocks):
    ny, nz = blocks.shape[:2]
    flat = blocks.reshape(ny * nz, *blocks.shape[2:])
    return lax.all_to_all(flat, BOTH, split_axis=0, concat_axis=0, tiled=True).reshape(blocks.shape)


def on_device(velocity, fluid, pressure):
    ny = lax.axis_size("py")
    nz = lax.axis_size("pz")
    _, depth, across = fluid.shape
    tz, ty = pressure.shape[1:]
    plane = depth * across * 4
    p4 = pressure.reshape(ny, nz, tz, ty)
    tiles = (ny, nz, tz, ty)
    sems = DMA((ny,))
    far = pltpu.HBM

    slab = (ny, depth, ty)
    packed, p_near, wz, wy = call(
        pack_kernel, [((ny, nz, 3, tz, ty), VMEM), (tiles, VMEM), (slab, VMEM), (slab, VMEM)],
        [(fluid.reshape(depth, across), far), (velocity.reshape(3, depth, across), far), (p4, far)],
        [VMEM((depth, across), F32)] * 2 + [DMA((4,)), DMA((4,)), DMA], 24, 9 * plane,
    )
    first = exchange(packed)
    op, faces, px = call(
        middle_kernel, [((ny, nz, 2, tz, ty), VMEM), ((3, depth, across), far), (tiles, VMEM)],
        [(first, VMEM), (p_near, VMEM), (wz, VMEM), (wy, VMEM), (velocity.reshape(3, depth, across), None)],
        [VMEM((2, depth, across), F32), DMA((4,))], 24, 7 * plane,
    )
    second = exchange(op)
    projected, divergence = call(
        final_kernel, [((3, nz, tz, across), far), (tiles, far)],
        [(second, VMEM), (px, VMEM), (faces.reshape(3, nz, tz, across), far)],
        [VMEM((nz, tz, across), F32), VMEM(tiles, F32), DMA((4,)), DMA((4,))], 16, 3 * plane,
        input_output_aliases={2: 0},
    )
    return projected.reshape(velocity.shape), divergence.reshape(pressure.shape)


def solution(mesh):
    placed = (P(None, BOTH, None, None), P(BOTH, None, None), P(None, "pz", "py"))
    return jax.shard_map(
        on_device,
        mesh=mesh,
        in_specs=placed,
        out_specs=(P(None, BOTH, None, None), P(None, "pz", "py")),
        check_vma=False,
    )
```

```python
import jax
import jax.numpy as jnp
from jax import lax
from jax.experimental import pallas as pl
from jax.experimental.pallas import tpu as pltpu
from jax.sharding import PartitionSpec as P

ANY = pl.ANY
BOTH = ("py", "pz")
F32 = jnp.float32
HBM = pl.BlockSpec(memory_space=pltpu.HBM)
VMEM = pltpu.VMEM
DMA = pltpu.SemaphoreType.DMA


def call(kernel, outs, ins, scratch, mib, moved, **more):
    spec = {ANY: HBM, pltpu.HBM: HBM, None: pl.BlockSpec(memory_space=VMEM), VMEM: pl.BlockSpec(memory_space=VMEM)}
    return pl.pallas_call(
        kernel,
        out_shape=tuple((space or jax.ShapeDtypeStruct)(shape, F32) for shape, space in outs),
        in_specs=[spec[space] for _, space in ins],
        out_specs=tuple(spec[space] for _, space in outs),
        scratch_shapes=scratch,
        compiler_params=pltpu.CompilerParams(vmem_limit_bytes=mib * 1024 * 1024),
        cost_estimate=pl.CostEstimate(flops=moved, bytes_accessed=moved, transcendentals=0),
        **more,
    )(*(x if space in (None, ANY) else pltpu.with_memory_space_constraint(x, space) for x, space in ins))


def start(copies):
    for c in copies:
        c.start()


def wait(copies):
    for c in copies:
        c.wait()


def pack_kernel(f_h, v_h, p_h, out, p, wz, wy, f, v, sem_f, sem_v, sem_p):
    ny, nz, _, tz, ty = out.shape
    copy = pltpu.make_async_copy
    part = nz // 4
    high = part * tz
    rows = [pl.ds(k * high, high) for k in range(4)]
    loads_f = [copy(f_h.at[k], f.at[k], sem_f.at[i]) for i, k in enumerate(rows)]
    loads_v = [copy(v_h.at[0, k], v.at[k], sem_v.at[i]) for i, k in enumerate(rows)]
    load_p = copy(p_h, p, sem_p)
    start(loads_f)
    load_p.start()
    start(loads_v)
    lane = lax.broadcasted_iota(jnp.int32, (high, ty), 1)
    for k in range(4):
        loads_f[k].wait()
        before = None
        for i in range(ny):
            cols = pl.ds(i * ty, ty)
            if k:
                tall = 0.5 * f[pl.ds(k * high - 8, high + 8), cols]
                half, above = tall[8:], pltpu.roll(tall, 1, 0)[8:]
                wz[i, rows[k]] = half + above
            else:
                half = 0.5 * f[rows[k], cols]
                row = lax.broadcasted_iota(jnp.int32, (high, ty), 0)
                wz[i, rows[k]] = jnp.where(row == 0, 0.0, half + pltpu.roll(half, 1, 0))
            out[i, k * part : (k + 1) * part, 0] = half.reshape(part, tz, ty)
            turned = pltpu.roll(half, 1, 1)
            if i:
                wy[i, rows[k]] = half + jnp.where(lane == 0, before, turned)
            else:
                wy[i, rows[k]] = jnp.where(lane == 0, 0.0, half + turned)
            before = turned
    load_p.wait()
    for i in range(ny):
        out[i, :, 2] = p[i]
    for k in range(4):
        loads_v[k].wait()
        for i in range(ny):
            out[i, k * part : (k + 1) * part, 1] = v[rows[k], pl.ds(i * ty, ty)].reshape(part, tz, ty)


def middle_kernel(r, p, wz, wy, v, op, proj_h, faces, sems):
    ny, nz, _, tz, ty = r.shape
    depth = nz * tz
    lane = lax.broadcasted_iota(jnp.int32, (depth, ty), 1)
    before = None
    stores = []
    for i in range(ny):
        cols = pl.ds(i * ty, ty)
        pres = r[i, :, 2].reshape(depth, ty)
        pz = wz[i] * (v[1, :, cols] - (pres - pltpu.roll(pres, 1, 0)))
        faces[0, :, cols] = pz
        dz = pltpu.roll(pz, depth - 1, 0) - pz
        rp = pltpu.roll(pres, 1, 1)
        left = jnp.where(lane == 0, before[0], rp) if i else rp
        py = wy[i] * (v[2, :, cols] - (pres - left))
        faces[1, :, cols] = py
        if i % 4 == 3 and i < ny - 1:
            done = pl.ds((i - 3) * ty, 4 * ty)
            stores.append(pltpu.make_async_copy(faces.at[:, :, done], proj_h.at[pl.ds(1, 2), :, done], sems.at[i // 4]))
            stores[-1].start()
        ry = pltpu.roll(py, ty - 1, 1)
        if i:
            op[i - 1, :, 1] = (before[2] + jnp.where(lane == ty - 1, ry, before[1])).reshape(nz, tz, ty)
        before = rp, ry, dz - py
    op[ny - 1, :, 1] = (before[2] + jnp.where(lane == ty - 1, 0.0, before[1])).reshape(nz, tz, ty)
    for i in range(ny):
        for j in range(nz):
            if i == 0 and j == 0:
                op[0, 0, 0] = jnp.zeros((tz, ty), F32)
                continue
            a, b = (i, j - 1) if j else (i - 1, nz - 1)
            weight = r[i, j, 0] + r[a, b, 0]
            op[i, j, 0] = weight * (r[i, j, 1] - (p[i, j] - p[a, b]))
    wait(stores)


def final_kernel(r, op, faces, partial, proj_h, div_h, first, div, sem_p, sem_d, sem_f):
    del partial
    ny, nz, _, tz, ty = r.shape
    copy = pltpu.make_async_copy
    part = nz // 4
    late = pl.ds((ny - 4) * ty, 4 * ty)
    stores = [copy(faces.at[:, :, :, late], proj_h.at[pl.ds(1, 2), :, :, late], sem_f)]
    start(stores)
    for k in range(4):
        for j in range(k * part, (k + 1) * part):
            for i in range(ny):
                first[j, :, i * ty : (i + 1) * ty] = r[i, j, 0]
        rows = pl.ds(k * part, part)
        stores.append(copy(first.at[rows], proj_h.at[0, rows], sem_p.at[k]))
        stores[-1].start()
    quarter = ny // 4
    for k in range(4):
        for i in range(k * quarter, (k + 1) * quarter):
            for j in range(nz):
                if j < nz - 1:
                    after = op[i, j + 1, 0]
                else:
                    after = op[i + 1, 0, 0] if i < ny - 1 else 0.0
                div[i, j] = r[i, j, 1] + (after - op[i, j, 0])
        rows = pl.ds(k * quarter, quarter)
        stores.append(copy(div.at[rows], div_h.at[rows], sem_d.at[k]))
        stores[-1].start()
    wait(stores)


def exchange(blocks):
    ny, nz = blocks.shape[:2]
    flat = blocks.reshape(ny * nz, *blocks.shape[2:])
    return lax.all_to_all(flat, BOTH, split_axis=0, concat_axis=0, tiled=True).reshape(blocks.shape)


def on_device(velocity, fluid, pressure):
    ny = lax.axis_size("py")
    nz = lax.axis_size("pz")
    _, depth, across = fluid.shape
    tz, ty = pressure.shape[1:]
    plane = depth * across * 4
    p4 = pressure.reshape(ny, nz, tz, ty)
    tiles = (ny, nz, tz, ty)
    sems = DMA((ny,))
    far = pltpu.HBM

    slab = (ny, depth, ty)
    packed, p_near, wz, wy = call(
        pack_kernel, [((ny, nz, 3, tz, ty), VMEM), (tiles, VMEM), (slab, VMEM), (slab, VMEM)],
        [(fluid.reshape(depth, across), far), (velocity.reshape(3, depth, across), far), (p4, far)],
        [VMEM((depth, across), F32)] * 2 + [DMA((4,)), DMA((4,)), DMA], 24, 9 * plane,
    )
    first = exchange(packed)
    op, partial, faces = call(
        middle_kernel, [((ny, nz, 2, tz, ty), VMEM), ((3, depth, across), far), ((2, depth, across), VMEM)],
        [(first, VMEM), (p_near, VMEM), (wz, VMEM), (wy, VMEM), (velocity.reshape(3, depth, across), None)],
        [DMA((4,))], 24, 7 * plane,
    )
    second = exchange(op)
    projected, divergence = call(
        final_kernel, [((3, nz, tz, across), far), (tiles, far)],
        [(second, VMEM), (op, VMEM), (faces.reshape(2, nz, tz, across), VMEM), (partial.reshape(3, nz, tz, across), far)],
        [VMEM((nz, tz, across), F32), VMEM(tiles, F32), DMA((4,)), DMA((4,)), DMA], 16, 3 * plane,
        input_output_aliases={3: 0},
    )
    return projected.reshape(velocity.shape), divergence.reshape(pressure.shape)


def solution(mesh):
    placed = (P(None, BOTH, None, None), P(BOTH, None, None), P(None, "pz", "py"))
    return jax.shard_map(
        on_device,
        mesh=mesh,
        in_specs=placed,
        out_specs=(P(None, BOTH, None, None), P(None, "pz", "py")),
        check_vma=False,
    )
```

```python
import jax
import jax.numpy as jnp
from jax import lax
from jax.experimental import pallas as pl
from jax.experimental.pallas import tpu as pltpu
from jax.sharding import PartitionSpec as P

ANY = pl.ANY
BOTH = ("py", "pz")
F32 = jnp.float32
HBM = pl.BlockSpec(memory_space=pltpu.HBM)
VMEM = pltpu.VMEM
DMA = pltpu.SemaphoreType.DMA


def call(kernel, outs, ins, scratch, mib, moved, **more):
    spec = {ANY: HBM, pltpu.HBM: HBM, None: pl.BlockSpec(memory_space=VMEM), VMEM: pl.BlockSpec(memory_space=VMEM)}
    return pl.pallas_call(
        kernel,
        out_shape=tuple((space or jax.ShapeDtypeStruct)(shape, F32) for shape, space in outs),
        in_specs=[spec[space] for _, space in ins],
        out_specs=tuple(spec[space] for _, space in outs),
        scratch_shapes=scratch,
        compiler_params=pltpu.CompilerParams(vmem_limit_bytes=mib * 1024 * 1024),
        cost_estimate=pl.CostEstimate(flops=moved, bytes_accessed=moved, transcendentals=0),
        **more,
    )(*(x if space in (None, ANY) else pltpu.with_memory_space_constraint(x, space) for x, space in ins))


def start(copies):
    for c in copies:
        c.start()


def wait(copies):
    for c in copies:
        c.wait()


def pack_kernel(f_h, v_h, p_h, out, wz, wy, f, sem_f, sem_v, sem_p):
    ny, nz, _, tz, ty = out.shape
    copy = pltpu.make_async_copy
    part = nz // 4
    high = part * tz
    rows = [pl.ds(k * high, high) for k in range(4)]
    loads_f = [copy(f_h.at[k], f.at[k], sem_f.at[i]) for i, k in enumerate(rows)]
    load_p = copy(p_h, out.at[:, :, 2], sem_p)
    loads_v = [copy(v_h.at[0, :, :, pl.ds(i * ty, ty)], out.at[i, :, 1], sem_v.at[i]) for i in range(ny)]
    start(loads_f)
    load_p.start()
    start(loads_v)
    lane = lax.broadcasted_iota(jnp.int32, (high, ty), 1)
    for k in range(4):
        loads_f[k].wait()
        before = None
        for i in range(ny):
            cols = pl.ds(i * ty, ty)
            if k:
                tall = 0.5 * f[pl.ds(k * high - 8, high + 8), cols]
                half, above = tall[8:], pltpu.roll(tall, 1, 0)[8:]
                wz[i, rows[k]] = half + above
            else:
                half = 0.5 * f[rows[k], cols]
                row = lax.broadcasted_iota(jnp.int32, (high, ty), 0)
                wz[i, rows[k]] = jnp.where(row == 0, 0.0, half + pltpu.roll(half, 1, 0))
            out[i, k * part : (k + 1) * part, 0] = half.reshape(part, tz, ty)
            turned = pltpu.roll(half, 1, 1)
            if i:
                wy[i, rows[k]] = half + jnp.where(lane == 0, before, turned)
            else:
                wy[i, rows[k]] = jnp.where(lane == 0, 0.0, half + turned)
            before = turned
    load_p.wait()
    wait(loads_v)


def middle_kernel(r, p, wz, wy, v, op, proj_h, faces, sems):
    ny, nz, _, tz, ty = r.shape
    depth = nz * tz
    lane = lax.broadcasted_iota(jnp.int32, (depth, ty), 1)
    before = None
    stores = []
    for i in range(ny):
        for j in range(nz):
            if i == 0 and j == 0:
                op[0, 0, 0] = jnp.zeros((tz, ty), F32)
                continue
            a, b = (i, j - 1) if j else (i - 1, nz - 1)
            weight = r[i, j, 0] + r[a, b, 0]
            op[i, j, 0] = weight * (r[i, j, 1] - (p[i, j] - p[a, b]))
        cols = pl.ds(i * ty, ty)
        pres = r[i, :, 2].reshape(depth, ty)
        pz = wz[i] * (v[1, :, cols] - (pres - pltpu.roll(pres, 1, 0)))
        faces[0, :, cols] = pz
        dz = pltpu.roll(pz, depth - 1, 0) - pz
        rp = pltpu.roll(pres, 1, 1)
        left = jnp.where(lane == 0, before[0], rp) if i else rp
        py = wy[i] * (v[2, :, cols] - (pres - left))
        faces[1, :, cols] = py
        if i % 4 == 3 and i < ny - 1:
            done = pl.ds((i - 3) * ty, 4 * ty)
            stores.append(pltpu.make_async_copy(faces.at[:, :, done], proj_h.at[pl.ds(1, 2), :, done], sems.at[i // 4]))
            stores[-1].start()
        ry = pltpu.roll(py, ty - 1, 1)
        if i:
            op[i - 1, :, 1] = (before[2] + jnp.where(lane == ty - 1, ry, before[1])).reshape(nz, tz, ty)
        before = rp, ry, dz - py
    op[ny - 1, :, 1] = (before[2] + jnp.where(lane == ty - 1, 0.0, before[1])).reshape(nz, tz, ty)
    wait(stores)


def final_kernel(r, op, faces, partial, proj_h, div_h, first, div, sem_p, sem_d, sem_f):
    del partial
    ny, nz, _, tz, ty = r.shape
    copy = pltpu.make_async_copy
    part = nz // 4
    late = pl.ds((ny - 4) * ty, 4 * ty)
    stores = [copy(faces.at[:, :, :, late], proj_h.at[pl.ds(1, 2), :, :, late], sem_f)]
    start(stores)
    for k in range(4):
        for j in range(k * part, (k + 1) * part):
            for i in range(ny):
                first[j, :, i * ty : (i + 1) * ty] = r[i, j, 0]
        rows = pl.ds(k * part, part)
        stores.append(copy(first.at[rows], proj_h.at[0, rows], sem_p.at[k]))
        stores[-1].start()
    quarter = ny // 4
    for k in range(4):
        for i in range(k * quarter, (k + 1) * quarter):
            for j in range(nz):
                if j < nz - 1:
                    after = op[i, j + 1, 0]
                else:
                    after = op[i + 1, 0, 0] if i < ny - 1 else 0.0
                div[i, j] = r[i, j, 1] + (after - op[i, j, 0])
        rows = pl.ds(k * quarter, quarter)
        stores.append(copy(div.at[rows], div_h.at[rows], sem_d.at[k]))
        stores[-1].start()
    wait(stores)


def exchange(blocks):
    ny, nz = blocks.shape[:2]
    flat = blocks.reshape(ny * nz, *blocks.shape[2:])
    return lax.all_to_all(flat, BOTH, split_axis=0, concat_axis=0, tiled=True).reshape(blocks.shape)


def on_device(velocity, fluid, pressure):
    ny = lax.axis_size("py")
    nz = lax.axis_size("pz")
    _, depth, across = fluid.shape
    tz, ty = pressure.shape[1:]
    plane = depth * across * 4
    p4 = pressure.reshape(ny, nz, tz, ty)
    tiles = (ny, nz, tz, ty)
    sems = DMA((ny,))
    far = pltpu.HBM

    slab = (ny, depth, ty)
    packed, wz, wy = call(
        pack_kernel, [((ny, nz, 3, tz, ty), VMEM), (slab, VMEM), (slab, VMEM)],
        [(fluid.reshape(depth, across), far), (velocity.reshape(3, nz, tz, across), far), (p4, far)],
        [VMEM((depth, across), F32), DMA((4,)), sems, DMA], 24, 9 * plane,
    )
    first = exchange(packed)
    op, partial, faces = call(
        middle_kernel, [((ny, nz, 2, tz, ty), VMEM), ((3, depth, across), far), ((2, depth, across), VMEM)],
        [(first, VMEM), (p4, None), (wz, VMEM), (wy, VMEM), (velocity.reshape(3, depth, across), None)],
        [DMA((4,))], 24, 7 * plane,
    )
    second = exchange(op)
    projected, divergence = call(
        final_kernel, [((3, nz, tz, across), far), (tiles, far)],
        [(second, VMEM), (op, VMEM), (faces.reshape(2, nz, tz, across), VMEM), (partial.reshape(3, nz, tz, across), far)],
        [VMEM((nz, tz, across), F32), VMEM(tiles, F32), DMA((4,)), DMA((4,)), DMA], 16, 3 * plane,
        input_output_aliases={3: 0},
    )
    return projected.reshape(velocity.shape), divergence.reshape(pressure.shape)


def solution(mesh):
    placed = (P(None, BOTH, None, None), P(BOTH, None, None), P(None, "pz", "py"))
    return jax.shard_map(
        on_device,
        mesh=mesh,
        in_specs=placed,
        out_specs=(P(None, BOTH, None, None), P(None, "pz", "py")),
        check_vma=False,
    )
```

```python
import jax
import jax.numpy as jnp
from jax import lax
from jax.experimental import pallas as pl
from jax.experimental.pallas import tpu as pltpu
from jax.sharding import PartitionSpec as P

ANY = pl.ANY
BOTH = ("py", "pz")
F32 = jnp.float32
HBM = pl.BlockSpec(memory_space=pltpu.HBM)
VMEM = pltpu.VMEM
DMA = pltpu.SemaphoreType.DMA


def call(kernel, outs, ins, scratch, mib, moved, **more):
    spec = {ANY: HBM, pltpu.HBM: HBM, None: pl.BlockSpec(memory_space=VMEM), VMEM: pl.BlockSpec(memory_space=VMEM)}
    return pl.pallas_call(
        kernel,
        out_shape=tuple((space or jax.ShapeDtypeStruct)(shape, F32) for shape, space in outs),
        in_specs=[spec[space] for _, space in ins],
        out_specs=tuple(spec[space] for _, space in outs),
        scratch_shapes=scratch,
        compiler_params=pltpu.CompilerParams(vmem_limit_bytes=mib * 1024 * 1024),
        cost_estimate=pl.CostEstimate(flops=moved, bytes_accessed=moved, transcendentals=0),
        **more,
    )(*(x if space in (None, ANY) else pltpu.with_memory_space_constraint(x, space) for x, space in ins))


def start(copies):
    for c in copies:
        c.start()


def wait(copies):
    for c in copies:
        c.wait()


def pack_kernel(f_h, v_h, p_h, out, wz, wy, f, sem_f, sem_v, sem_p):
    ny, nz, _, tz, ty = out.shape
    copy = pltpu.make_async_copy
    part = nz // 4
    high = part * tz
    rows = [pl.ds(k * high, high) for k in range(4)]
    loads_f = [copy(f_h.at[k], f.at[k], sem_f.at[i]) for i, k in enumerate(rows)]
    load_p = copy(p_h, out.at[:, :, 2], sem_p)
    loads_v = [copy(v_h.at[0, :, :, pl.ds(i * ty, ty)], out.at[i, :, 1], sem_v.at[i]) for i in range(ny)]
    start(loads_f)
    load_p.start()
    start(loads_v)
    lane = lax.broadcasted_iota(jnp.int32, (high, ty), 1)
    for k in range(4):
        loads_f[k].wait()
        before = None
        for i in range(ny):
            cols = pl.ds(i * ty, ty)
            if k:
                tall = 0.5 * f[pl.ds(k * high - 8, high + 8), cols]
                half, above = tall[8:], pltpu.roll(tall, 1, 0)[8:]
                wz[i, rows[k]] = half + above
            else:
                half = 0.5 * f[rows[k], cols]
                row = lax.broadcasted_iota(jnp.int32, (high, ty), 0)
                wz[i, rows[k]] = jnp.where(row == 0, 0.0, half + pltpu.roll(half, 1, 0))
            out[i, k * part : (k + 1) * part, 0] = half.reshape(part, tz, ty)
            turned = pltpu.roll(half, 1, 1)
            if i:
                wy[i, rows[k]] = half + jnp.where(lane == 0, before, turned)
            else:
                wy[i, rows[k]] = jnp.where(lane == 0, 0.0, half + turned)
            before = turned
    load_p.wait()
    wait(loads_v)


def middle_kernel(r, p, wz, wy, v, op, proj_h, faces, sems):
    ny, nz, _, tz, ty = r.shape
    depth = nz * tz
    lane = lax.broadcasted_iota(jnp.int32, (depth, ty), 1)
    before = None
    stores = []
    for i in range(ny):
        for j in range(nz):
            if i == 0 and j == 0:
                op[0, 0, 0] = jnp.zeros((tz, ty), F32)
                continue
            a, b = (i, j - 1) if j else (i - 1, nz - 1)
            weight = r[i, j, 0] + r[a, b, 0]
            op[i, j, 0] = weight * (r[i, j, 1] - (p[i, j] - p[a, b]))
        cols = pl.ds(i * ty, ty)
        pres = r[i, :, 2].reshape(depth, ty)
        pz = wz[i] * (v[1, :, cols] - (pres - pltpu.roll(pres, 1, 0)))
        faces[0, :, cols] = pz
        dz = pltpu.roll(pz, depth - 1, 0) - pz
        rp = pltpu.roll(pres, 1, 1)
        left = jnp.where(lane == 0, before[0], rp) if i else rp
        py = wy[i] * (v[2, :, cols] - (pres - left))
        faces[1, :, cols] = py
        if i % 4 == 3 and i < ny // 2:
            done = pl.ds((i - 3) * ty, 4 * ty)
            stores.append(pltpu.make_async_copy(faces.at[:, :, done], proj_h.at[pl.ds(1, 2), :, done], sems.at[i // 4]))
            stores[-1].start()
        ry = pltpu.roll(py, ty - 1, 1)
        if i:
            op[i - 1, :, 1] = (before[2] + jnp.where(lane == ty - 1, ry, before[1])).reshape(nz, tz, ty)
        before = rp, ry, dz - py
    op[ny - 1, :, 1] = (before[2] + jnp.where(lane == ty - 1, 0.0, before[1])).reshape(nz, tz, ty)
    wait(stores)


def final_kernel(r, op, faces, partial, proj_h, div_h, first, div, sem_p, sem_d, sem_f):
    del partial
    ny, nz, _, tz, ty = r.shape
    copy = pltpu.make_async_copy
    part = nz // 4
    late = pl.ds(ny // 2 * ty, ny // 2 * ty)
    stores = [copy(faces.at[:, :, :, late], proj_h.at[pl.ds(1, 2), :, :, late], sem_f)]
    start(stores)
    for k in range(4):
        for j in range(k * part, (k + 1) * part):
            for i in range(ny):
                first[j, :, i * ty : (i + 1) * ty] = r[i, j, 0]
        rows = pl.ds(k * part, part)
        stores.append(copy(first.at[rows], proj_h.at[0, rows], sem_p.at[k]))
        stores[-1].start()
    quarter = ny // 4
    for k in range(4):
        for i in range(k * quarter, (k + 1) * quarter):
            for j in range(nz):
                if j < nz - 1:
                    after = op[i, j + 1, 0]
                else:
                    after = op[i + 1, 0, 0] if i < ny - 1 else 0.0
                div[i, j] = r[i, j, 1] + (after - op[i, j, 0])
        rows = pl.ds(k * quarter, quarter)
        stores.append(copy(div.at[rows], div_h.at[rows], sem_d.at[k]))
        stores[-1].start()
    wait(stores)


def exchange(blocks):
    ny, nz = blocks.shape[:2]
    flat = blocks.reshape(ny * nz, *blocks.shape[2:])
    return lax.all_to_all(flat, BOTH, split_axis=0, concat_axis=0, tiled=True).reshape(blocks.shape)


def on_device(velocity, fluid, pressure):
    ny = lax.axis_size("py")
    nz = lax.axis_size("pz")
    _, depth, across = fluid.shape
    tz, ty = pressure.shape[1:]
    plane = depth * across * 4
    p4 = pressure.reshape(ny, nz, tz, ty)
    tiles = (ny, nz, tz, ty)
    sems = DMA((ny,))
    far = pltpu.HBM

    slab = (ny, depth, ty)
    packed, wz, wy = call(
        pack_kernel, [((ny, nz, 3, tz, ty), VMEM), (slab, VMEM), (slab, VMEM)],
        [(fluid.reshape(depth, across), far), (velocity.reshape(3, nz, tz, across), far), (p4, far)],
        [VMEM((depth, across), F32), DMA((4,)), sems, DMA], 24, 9 * plane,
    )
    first = exchange(packed)
    op, partial, faces = call(
        middle_kernel, [((ny, nz, 2, tz, ty), VMEM), ((3, depth, across), far), ((2, depth, across), VMEM)],
        [(first, VMEM), (p4, None), (wz, VMEM), (wy, VMEM), (velocity.reshape(3, depth, across), None)],
        [DMA((4,))], 24, 7 * plane,
    )
    second = exchange(op)
    projected, divergence = call(
        final_kernel, [((3, nz, tz, across), far), (tiles, far)],
        [(second, VMEM), (op, VMEM), (faces.reshape(2, nz, tz, across), VMEM), (partial.reshape(3, nz, tz, across), far)],
        [VMEM((nz, tz, across), F32), VMEM(tiles, F32), DMA((4,)), DMA((4,)), DMA], 16, 3 * plane,
        input_output_aliases={3: 0},
    )
    return projected.reshape(velocity.shape), divergence.reshape(pressure.shape)


def solution(mesh):
    placed = (P(None, BOTH, None, None), P(BOTH, None, None), P(None, "pz", "py"))
    return jax.shard_map(
        on_device,
        mesh=mesh,
        in_specs=placed,
        out_specs=(P(None, BOTH, None, None), P(None, "pz", "py")),
        check_vma=False,
    )
```
